32 devices in a mesh: freq: 2 (over x), param: 4 (over y, core), sens: 4 (over z).
Axes of the slice: x: 2, y: 2, z: 4, core: 2. Of those that a mesh axis runs over, the one named last changes fastest.
Arguments:
- series: bfloat16 [8, 600, 52], P(None, 'sens', 'freq'), may hold values from -6 to 6
- kernel: bfloat16 [2, 32, 600, 4096], P(None, 'freq', 'sens', 'param'), may hold values from -0.1875 to 0.1875
- prior_spectrum: float32 [32], P('freq'), may hold values from 0.3 to 1.5
- prior_scale: float32 [4096], P('param'), may hold values from 0.5 to 2
Outputs:
- adjoint_map: float32 [52, 8, 4096], P('freq', 'sens', 'param')
The draws below stay inside these ranges and needn't reach their ends.
All inputs are finite; a program needn't handle non-finite values.
Results may differ from the reference program's by a relative error of at most 0.0047.
Values may be sent and summed in bfloat16 or wider, within the bound.
A program may use at most 64 MiB of HBM per device.

```python
import math
import jax
import jax.numpy as jnp
from jax import lax

SENSORS = 600
LEN = 840
NB = 32
NT = 52
NP = 4096
PROBES = 8


def level_of(rng, extent, pieces, smallest, high):
    def one(position, blocks):
        steps = jax.random.uniform(jax.random.fold_in(jax.random.fold_in(rng, 6), position), (blocks,), jnp.float32, smallest / len(pieces), high / len(pieces))
        return jnp.repeat(jnp.exp(steps), extent[position] // blocks).reshape((-1,) + (1,) * (len(extent) - position - 1))

    level = one(*pieces[0])
    for cut in pieces[1:]:
        level = level * one(*cut)
    return level


def noise(rng, extent, width, reach, cuts=(), kind=jnp.bfloat16):
    entries = jax.random.normal(rng, extent, jnp.float32) * width
    if len(cuts) > 0:
        entries = level_of(rng, extent, cuts, -0.22, 0.18) * entries
    return jnp.clip(entries, min=-reach, max=reach).astype(kind)


def setup_inputs(seed: int = 0) -> dict:
    key_of = jax.random.split(jax.random.key(seed), 5)
    series = noise(key_of[0], (PROBES, SENSORS, NT), 1.0, 6.0, ((1, 4), (2, 2)))
    kernel = noise(key_of[1], (2, NB, SENSORS, NP), (2 * SENSORS) ** -0.5, 0.1875, ((1, 2), (2, 4), (3, 4)))
    prior_spectrum = jnp.clip(jnp.exp(math.log(1.5) - 1.60943787 * jax.random.uniform(key_of[2], (NB,), jnp.float32) ** level_of(key_of[2], (NB,), ((0, 2),), -0.2, 0.2)), 0.3, 1.5)
    prior_scale = jnp.clip(jnp.exp(math.log(2.0) - 1.3862944 * jax.random.uniform(key_of[3], (NP,), jnp.float32) ** level_of(key_of[3], (NP,), ((0, 4),), -0.2, 0.2)), 0.5, 2.0)
    return {"series": series, "kernel": kernel, "prior_spectrum": prior_spectrum, "prior_scale": prior_scale}


def phase_tables(bin_count, time_count):
    bin_index = jnp.arange(bin_count, dtype=jnp.int32)
    time_index = jnp.arange(time_count, dtype=jnp.int32)
    product = time_index[:, None] * bin_index[None, :] % LEN
    phase_angle = product.astype(jnp.float32) * (2.0 * math.pi / LEN)
    return (jnp.cos(phase_angle), jnp.sin(phase_angle))

def reference(series, kernel, prior_spectrum, prior_scale):
    highest = lax.Precision.HIGHEST
    cosine, sine_part = phase_tables(NB, NT)
    flat_rows = series.astype(jnp.float32).reshape(PROBES * SENSORS, NT)
    norm_time = 1.0 / math.sqrt(NT)
    spec_re = (jnp.dot(flat_rows, cosine, precision=highest) * norm_time).astype(jnp.bfloat16)
    spec_im = (-jnp.dot(flat_rows, sine_part, precision=highest) * norm_time).astype(jnp.bfloat16)
    spec_re = spec_re.reshape(PROBES, SENSORS, NB).transpose(2, 1, 0)
    spec_im = spec_im.reshape(PROBES, SENSORS, NB).transpose(2, 1, 0)

    def one_bin(index):
        kern_re = kernel[0, index]
        kern_im = kernel[1, index]
        data_re = spec_re[index].T
        data_im = spec_im[index].T
        real_part = jnp.dot(data_re, kern_re, preferred_element_type=jnp.float32) + jnp.dot(data_im, kern_im, preferred_element_type=jnp.float32)
        imag_part = jnp.dot(data_im, kern_re, preferred_element_type=jnp.float32) - jnp.dot(data_re, kern_im, preferred_element_type=jnp.float32)
        return jnp.stack([real_part, imag_part])
    spectra = lax.map(one_bin, jnp.arange(NB, dtype=jnp.int32))
    weights = prior_spectrum / math.sqrt(NB)
    scaled_spec = spectra * weights[:, None, None, None]
    image_re = scaled_spec[:, 0].reshape(NB, PROBES * NP)
    image_im = scaled_spec[:, 1].reshape(NB, PROBES * NP)
    image_field = jnp.dot(cosine, image_re, precision=highest) - jnp.dot(sine_part, image_im, precision=highest)
    image_field = image_field.reshape(NT, PROBES, NP)
    weighted = image_field * prior_scale
    padded = jnp.pad(weighted, ((0, 0), (0, 0), (1, 1)))
    smooth = 0.5 * weighted + 0.25 * (padded[:, :, :-2] + padded[:, :, 2:])
    return smooth * prior_scale
```

```python
import functools
import math

import jax
import jax.numpy as jnp
import numpy as np
from jax import lax
from jax.experimental import pallas as pl
from jax.experimental.pallas import tpu as pltpu
from jax.sharding import PartitionSpec as P

LEN = 840
MESH = pl.DeviceIdType.MESH
BF16 = jnp.bfloat16
F32 = jnp.float32


def split(table):
    high = table.astype(BF16)
    low = (table - high.astype(np.float32)).astype(BF16)
    return high, low


def trig(bins, times):
    angle = 2.0 * np.pi * ((np.arange(times)[:, None] * np.arange(bins)[None, :]) % LEN) / LEN
    return np.cos(angle), np.sin(angle)


def spectrum_tables(groups, bins_dev, time_dev, probes):
    cosine, sine = trig(groups * bins_dev, groups * time_dev)
    scale = 1.0 / math.sqrt(groups * time_dev)
    both = np.stack([cosine, -sine], axis=0) * scale
    both = both.reshape(2, groups * time_dev, groups, bins_dev).transpose(2, 0, 3, 1)
    flat = np.repeat(both.reshape(groups, 2 * bins_dev, -1), probes, axis=-1).astype(np.float32)
    high, low = split(flat)
    return np.stack([high, low], axis=1)


def pick_tables(bins_dev, senses, keep):
    split_by = (bins_dev // 8, senses, 8, 2, keep)
    half, _, inner, part, _ = np.indices(split_by).reshape(len(split_by), -1)
    rows = np.arange(half.size)
    bins = half * 8 + inner
    first = np.zeros((half.size, 2 * bins_dev), np.float32)
    second = np.zeros_like(first)
    first[rows, part * bins_dev + bins] = 1.0
    second[rows, (1 - part) * bins_dev + bins] = np.where(part == 0, 1.0, -1.0)
    return np.stack([first, second]).astype(BF16)


def image_tables(groups, bins_dev, time_dev, keep):
    cosine, sine = trig(groups * bins_dev, groups * time_dev)
    both = np.stack([cosine, -sine], axis=2).reshape(groups, time_dev, groups, bins_dev, 2)
    both = both.transpose(2, 0, 1, 3, 4)
    full = np.einsum("ghtbc,qr->ghtqbcr", both, np.eye(keep)).astype(np.float32)
    flat = full.reshape(groups, groups, time_dev * keep, bins_dev * 2 * keep)
    high, low = split(flat)
    return np.concatenate([high, low, high], axis=-1)


def body(
    cfg,
    series_hbm,
    kernel_hbm,
    prior_hbm,
    scale_hbm,
    spec_hbm,
    img_hbm,
    pick_hbm,
    out_ref,
    kbuf,
    prior,
    scale,
    spec_tab,
    img_tab,
    pick,
    gathered,
    wide,
    spread,
    left_mat,
    weight,
    sbuf,
    rbuf,
    own,
    xsend,
    xrecv,
    halo_left,
    halo_right,
    small_sem,
    k_sem,
    g_send,
    g_recv,
    z_send,
    z_recv,
    x_send,
    x_recv,
    hl_send,
    hl_recv,
    hr_send,
    hr_recv,
):
    groups, params, senses, chunks = cfg
    f = lax.axis_index("freq")
    k = lax.axis_index("param")
    s = lax.axis_index("sens")
    _, sens_dev, bins_dev, _ = kernel_hbm.shape
    halves = bins_dev // 8
    width = kbuf.shape[-1]
    block = wide.shape[2] // halves
    probes = block // 16
    keep = probes // senses
    edge = halo_left.shape[-1]

    def freq_peer(d):
        return lax.rem(f + d, groups)

    def sens_peer(d):
        return lax.rem(s + d, senses)

    small = [
        pltpu.make_async_copy(series_hbm, gathered.at[f], small_sem.at[0]),
        pltpu.make_async_copy(spec_hbm.at[f], spec_tab, small_sem.at[1]),
        pltpu.make_async_copy(prior_hbm, prior, small_sem.at[2]),
        pltpu.make_async_copy(scale_hbm, scale, small_sem.at[3]),
        pltpu.make_async_copy(img_hbm.at[f], img_tab, small_sem.at[4]),
        pltpu.make_async_copy(pick_hbm, pick, small_sem.at[5]),
    ]
    for copy in small:
        copy.start()
    loads = [
        [
            pltpu.make_async_copy(
                kernel_hbm.at[part, :, pl.ds(h * 8, 8), pl.ds(c * width, width)],
                kbuf.at[c, part, h],
                k_sem.at[c, part, h],
            )
            for h in range(halves)
            for part in range(2)
        ]
        for c in range(chunks)
    ]
    for group in loads:
        for copy in group:
            copy.start()

    barrier = pltpu.get_barrier_semaphore()
    for d in range(1, groups):
        pl.semaphore_signal(
            barrier, inc=1, device_id={"freq": freq_peer(d)}, device_id_type=MESH
        )
    for d in range(1, senses):
        pl.semaphore_signal(
            barrier, inc=1, device_id={"sens": sens_peer(d)}, device_id_type=MESH
        )
    has_left = k > 0
    has_right = k < params - 1

    @pl.when(has_left)
    def _():
        for d in range(groups):
            pl.semaphore_signal(
                barrier,
                inc=1,
                device_id={"freq": freq_peer(d), "param": k - 1},
                device_id_type=MESH,
            )

    @pl.when(has_right)
    def _():
        for d in range(groups):
            pl.semaphore_signal(
                barrier,
                inc=1,
                device_id={"freq": freq_peer(d), "param": k + 1},
                device_id_type=MESH,
            )

    small[0].wait()
    peers = groups + senses - 2
    beside = jnp.where(has_left, groups, 0) + jnp.where(has_right, groups, 0)
    pl.semaphore_wait(barrier, peers + beside)

    def series_copy(slot, target):
        return pltpu.make_async_remote_copy(
            src_ref=gathered.at[f],
            dst_ref=gathered.at[slot],
            send_sem=g_send.at[target],
            recv_sem=g_recv.at[slot],
            device_id={"freq": target},
            device_id_type=MESH,
        )

    for d in range(1, groups):
        series_copy(f, freq_peer(d)).start()
    for copy in small[1:]:
        copy.wait()
    probe_row = wide.shape[2]
    row = lax.broadcasted_iota(jnp.int32, (probe_row, wide.shape[3]), 0)
    lane = lax.broadcasted_iota(jnp.int32, (probe_row, wide.shape[3]), 1)
    probe = (row // (16 * keep)) % senses * keep + row % keep
    same = lane % probes == probe
    for v in range(2):
        for i in range(2):
            full = jnp.dot(pick[v], spec_tab[i], preferred_element_type=F32)
            wide[v, i] = jnp.where(same, full, 0.0).astype(BF16)
    row = lax.broadcasted_iota(jnp.int32, spread.shape, 0)
    lane = lax.broadcasted_iota(jnp.int32, spread.shape, 1)
    spread[...] = jnp.where(lane // 8 == row, 1.0, 0.0).astype(BF16)
    norm = 1.0 / math.sqrt(bins_dev * groups)
    row = lax.broadcasted_iota(jnp.int32, weight.shape[1:], 0)
    for h in range(halves):
        value = jnp.zeros(weight.shape[1:], F32)
        for b in range(8):
            value = jnp.where(row // (2 * keep) == b, prior[h * 8 + b] * norm, value)
        weight[h] = value

    for d in range(1, groups):
        series_copy(freq_peer(d), freq_peer(d)).wait_recv()
    rows = jnp.concatenate([gathered[g] for g in range(groups)], axis=0)
    row = lax.broadcasted_iota(jnp.int32, (block, spread.shape[1]), 0)
    lane = lax.broadcasted_iota(jnp.int32, (block, spread.shape[1]), 1)
    same = lane % 8 == row // (2 * keep) % 8
    for h in range(halves):
        for v in range(2):
            spec = jnp.dot(
                wide[v, 0, h * block : (h + 1) * block], rows, preferred_element_type=F32
            ) + jnp.dot(
                wide[v, 1, h * block : (h + 1) * block], rows, preferred_element_type=F32
            )
            full = jnp.dot(spec.astype(BF16), spread[...], preferred_element_type=F32)
            left_mat[v, h] = jnp.where(same, full, 0.0).astype(BF16)


    def z_copy(target, slot, c):
        return pltpu.make_async_remote_copy(
            src_ref=sbuf.at[target, c],
            dst_ref=rbuf.at[slot, c],
            send_sem=z_send.at[target, c],
            recv_sem=z_recv.at[slot, c],
            device_id={"sens": target},
            device_id_type=MESH,
        )

    for c in range(chunks):
        for h in range(halves):
            total = jnp.zeros((block, width), F32)
            for part in range(2):
                loads[c][h * 2 + part].wait()
                right_mat = kbuf.at[c, part, h].reshape(sens_dev * 8, width)[...]
                total = total + jnp.dot(
                    left_mat[part, h], right_mat, preferred_element_type=F32
                )
            each = block // senses
            for j in range(senses):
                piece = total[j * each : (j + 1) * each] * weight[h]
                sbuf[j, c, h * each : (h + 1) * each, :] = piece.astype(BF16)
        for d in (2, 1, 3) if senses == 4 else range(1, senses):
            z_copy(sens_peer(d), s, c).start()

    def x_copy(target, slot, c):
        return pltpu.make_async_remote_copy(
            src_ref=xsend.at[target, c],
            dst_ref=xrecv.at[slot, c],
            send_sem=x_send.at[target, c],
            recv_sem=x_recv.at[slot, c],
            device_id={"freq": target},
            device_id_type=MESH,
        )

    def to_left(target, slot):
        return pltpu.make_async_remote_copy(
            src_ref=xsend.at[target, 0, :, pl.ds(0, edge)],
            dst_ref=halo_right.at[slot],
            send_sem=hl_send.at[target],
            recv_sem=hr_recv.at[slot],
            device_id={"freq": target, "param": jnp.maximum(k - 1, 0)},
            device_id_type=MESH,
        )

    def to_right(target, slot):
        return pltpu.make_async_remote_copy(
            src_ref=xsend.at[target, chunks - 1, :, pl.ds(width - edge, edge)],
            dst_ref=halo_left.at[slot],
            send_sem=hr_send.at[target],
            recv_sem=hl_recv.at[slot],
            device_id={"freq": target, "param": jnp.minimum(k + 1, params - 1)},
            device_id_type=MESH,
        )

    for c in range(chunks):
        total = sbuf[s, c].astype(F32)
        for d in range(1, senses):
            z_copy(sens_peer(d), sens_peer(d), c).wait_recv()
            total = total + rbuf[sens_peer(d), c].astype(F32)
        high = total.astype(BF16)
        low = (total - high.astype(F32)).astype(BF16)
        stacked = jnp.concatenate([high, high, low], axis=0)
        lanes = scale[:, c * width : (c + 1) * width]
        for d in list(range(1, groups)) + [0]:
            g = freq_peer(d)
            image = jnp.dot(img_tab[g], stacked, preferred_element_type=F32) * lanes
            if d == 0:
                own[c] = image
                if c == 0 or c == chunks - 1:
                    xsend[g, c] = image.astype(BF16)
            else:
                xsend[g, c] = image.astype(BF16)
                x_copy(g, f, c).start()
        if c == 0:

            @pl.when(has_left)
            def _():
                for d in range(groups):
                    to_left(freq_peer(d), f).start()

        if c == chunks - 1:

            @pl.when(has_right)
            def _():
                for d in range(groups):
                    to_right(freq_peer(d), f).start()

    for c in range(chunks):
        image = own[c]
        for d in range(1, groups):
            g = freq_peer(d)
            x_copy(g, g, c).wait_recv()
            image = image + xrecv[g, c].astype(F32)
        own[c] = image


    @pl.when(has_left)
    def _():
        for d in range(groups):
            to_right(freq_peer(d), freq_peer(d)).wait_recv()

    @pl.when(jnp.logical_not(has_left))
    def _():
        halo_left[...] = jnp.zeros_like(halo_left)

    @pl.when(has_right)
    def _():
        for d in range(groups):
            to_left(freq_peer(d), freq_peer(d)).wait_recv()

    @pl.when(jnp.logical_not(has_right))
    def _():
        halo_right[...] = jnp.zeros_like(halo_right)

    left = halo_left[0].astype(F32)
    right = halo_right[0].astype(F32)
    for g in range(1, groups):
        left = left + halo_left[g].astype(F32)
        right = right + halo_right[g].astype(F32)
    for c in range(chunks):
        mid = own[c]
        before = own[c - 1][:, width - 1 :] if c > 0 else left[:, edge - 1 :]
        after = own[c + 1][:, :1] if c < chunks - 1 else right[:, :1]
        lower = jnp.concatenate([before, mid[:, :-1]], axis=1)
        upper = jnp.concatenate([mid[:, 1:], after], axis=1)
        lanes = scale[:, c * width : (c + 1) * width]
        out_ref[:, c * width : (c + 1) * width] = lanes * (0.5 * mid + 0.25 * (lower + upper))

    for d in range(1, groups):
        series_copy(f, freq_peer(d)).wait_send()
        for c in range(chunks):
            x_copy(freq_peer(d), f, c).wait_send()
    for c in range(chunks):
        for d in range(1, senses):
            z_copy(sens_peer(d), s, c).wait_send()

    @pl.when(has_left)
    def _():
        for d in range(groups):
            to_left(freq_peer(d), f).wait_send()

    @pl.when(has_right)
    def _():
        for d in range(groups):
            to_right(freq_peer(d), f).wait_send()


def local(mesh_shape, series, kernel, prior_spectrum, prior_scale):
    groups, params, senses = (mesh_shape[n] for n in ("freq", "param", "sens"))
    probes, sens_dev, time_dev = series.shape
    _, bins_dev, _, cols = kernel.shape
    keep = probes // senses
    chunks = 4
    width = cols // chunks
    edge = min(128, width)
    rows = time_dev * keep
    depth = bins_dev * 2 * keep
    halves = bins_dev // 8
    block = 16 * probes
    spec_tab = spectrum_tables(groups, bins_dev, time_dev, probes)
    pick_tab = pick_tables(bins_dev, senses, keep)
    img_tab = image_tables(groups, bins_dev, time_dev, keep)
    dma = pltpu.SemaphoreType.DMA
    out = pl.pallas_call(
        functools.partial(body, (groups, params, senses, chunks)),
        out_shape=jax.ShapeDtypeStruct((rows, cols), F32),
        in_specs=[pl.BlockSpec(memory_space=pltpu.HBM)] * 7,
        out_specs=pl.BlockSpec(memory_space=pltpu.VMEM),
        scratch_shapes=[
            pltpu.VMEM((chunks, 2, halves, sens_dev, 8, width), BF16),
            pltpu.SMEM((bins_dev,), F32),
            pltpu.VMEM((1, cols), F32),
            pltpu.VMEM(spec_tab.shape[1:], BF16),
            pltpu.VMEM(img_tab.shape[1:], BF16),
            pltpu.VMEM(pick_tab.shape, BF16),
            pltpu.VMEM((groups, time_dev * probes, sens_dev), BF16),
            pltpu.VMEM((2, 2, halves * block, groups * time_dev * probes), BF16),
            pltpu.VMEM((sens_dev, sens_dev * 8), BF16),
            pltpu.VMEM((2, halves, block, sens_dev * 8), BF16),
            pltpu.VMEM((halves, block // senses, width), F32),
            pltpu.VMEM((senses, chunks, depth, width), BF16),
            pltpu.VMEM((senses, chunks, depth, width), BF16),
            pltpu.VMEM((chunks, rows, width), F32),
            pltpu.VMEM((groups, chunks, rows, width), BF16),
            pltpu.VMEM((groups, chunks, rows, width), BF16),
            pltpu.VMEM((groups, rows, edge), BF16),
            pltpu.VMEM((groups, rows, edge), BF16),
            dma((6,)),
            dma((chunks, 2, halves)),
            dma((groups,)),
            dma((groups,)),
            dma((senses, chunks)),
            dma((senses, chunks)),
            dma((groups, chunks)),
            dma((groups, chunks)),
            dma((groups,)),
            dma((groups,)),
            dma((groups,)),
            dma((groups,)),
        ],
        compiler_params=pltpu.CompilerParams(
            collective_id=0, has_side_effects=True, vmem_limit_bytes=60 * 1024 * 1024
        ),
    )(
        series.transpose(2, 0, 1).reshape(time_dev * probes, sens_dev),
        kernel.transpose(0, 2, 1, 3),
        prior_spectrum,
        prior_scale.reshape(1, cols),
        jnp.asarray(spec_tab),
        jnp.asarray(img_tab),
        jnp.asarray(pick_tab),
    )
    return out.reshape(time_dev, keep, cols)


def solution(mesh):
    placed = (P(None, "sens", "freq"), P(None, "freq", "sens", "param"), P("freq"), P("param"))
    return jax.shard_map(
        functools.partial(local, dict(mesh.shape)),
        mesh=mesh,
        in_specs=placed,
        out_specs=P("freq", "sens", "param"),
        check_vma=False,
    )
```

```python
import functools
import math

import jax
import jax.numpy as jnp
import numpy as np
from jax import lax
from jax.experimental import pallas as pl
from jax.experimental.pallas import tpu as pltpu
from jax.sharding import PartitionSpec as P

LEN = 840
MESH = pl.DeviceIdType.MESH
BF16 = jnp.bfloat16
F32 = jnp.float32


def split(table):
    high = table.astype(BF16)
    low = (table - high.astype(np.float32)).astype(BF16)
    return high, low


def trig(bins, times):
    angle = 2.0 * np.pi * ((np.arange(times)[:, None] * np.arange(bins)[None, :]) % LEN) / LEN
    return np.cos(angle), np.sin(angle)


def spectrum_tables(groups, bins_dev, time_dev, probes):
    cosine, sine = trig(groups * bins_dev, groups * time_dev)
    scale = 1.0 / math.sqrt(groups * time_dev)
    both = np.stack([cosine, -sine], axis=0) * scale
    both = both.reshape(2, groups * time_dev, groups, bins_dev).transpose(2, 0, 3, 1)
    flat = np.repeat(both.reshape(groups, 2 * bins_dev, -1), probes, axis=-1).astype(np.float32)
    high, low = split(flat)
    return np.stack([high, low], axis=1)


def pick_tables(bins_dev, senses, keep):
    split_by = (bins_dev // 8, senses, 8, 2, keep)
    half, _, inner, part, _ = np.indices(split_by).reshape(len(split_by), -1)
    rows = np.arange(half.size)
    bins = half * 8 + inner
    first = np.zeros((half.size, 2 * bins_dev), np.float32)
    second = np.zeros_like(first)
    first[rows, part * bins_dev + bins] = 1.0
    second[rows, (1 - part) * bins_dev + bins] = np.where(part == 0, 1.0, -1.0)
    return np.stack([first, second]).astype(BF16)


def image_tables(groups, bins_dev, time_dev, keep):
    cosine, sine = trig(groups * bins_dev, groups * time_dev)
    both = np.stack([cosine, -sine], axis=2).reshape(groups, time_dev, groups, bins_dev, 2)
    both = both.transpose(2, 0, 1, 3, 4)
    full = np.einsum("ghtbc,qr->ghtqbcr", both, np.eye(keep)).astype(np.float32)
    flat = full.reshape(groups, groups, time_dev * keep, bins_dev * 2 * keep)
    high, low = split(flat)
    return np.concatenate([high, low, high], axis=-1)


def body(
    cfg,
    series_hbm,
    kernel_hbm,
    prior_hbm,
    scale_hbm,
    spec_hbm,
    img_hbm,
    pick_hbm,
    out_ref,
    kbuf,
    prior,
    scale,
    spec_tab,
    img_tab,
    pick,
    gathered,
    wide,
    spread,
    left_mat,
    weight,
    sbuf,
    rbuf,
    relay,
    joined,
    own,
    xsend,
    xrecv,
    halo_left,
    halo_right,
    small_sem,
    k_sem,
    g_send,
    g_recv,
    z_send,
    z_recv,
    relay_send,
    relay_recv,
    x_send,
    x_recv,
    hl_send,
    hl_recv,
    hr_send,
    hr_recv,
):
    groups, params, senses, chunks = cfg
    f = lax.axis_index("freq")
    k = lax.axis_index("param")
    s = lax.axis_index("sens")
    _, sens_dev, bins_dev, _ = kernel_hbm.shape
    halves = bins_dev // 8
    width = kbuf.shape[-1]
    block = wide.shape[2] // halves
    probes = block // 16
    keep = probes // senses
    edge = halo_left.shape[-1]

    def freq_peer(d):
        return lax.rem(f + d, groups)

    def sens_peer(d):
        return lax.rem(s + d, senses)

    small = [
        pltpu.make_async_copy(series_hbm, gathered.at[f], small_sem.at[0]),
        pltpu.make_async_copy(spec_hbm.at[f], spec_tab, small_sem.at[1]),
        pltpu.make_async_copy(prior_hbm, prior, small_sem.at[2]),
        pltpu.make_async_copy(scale_hbm, scale, small_sem.at[3]),
        pltpu.make_async_copy(img_hbm.at[f], img_tab, small_sem.at[4]),
        pltpu.make_async_copy(pick_hbm, pick, small_sem.at[5]),
    ]
    for copy in small:
        copy.start()
    loads = [
        [
            pltpu.make_async_copy(
                kernel_hbm.at[part, :, pl.ds(h * 8, 8), pl.ds(c * width, width)],
                kbuf.at[c, part, h],
                k_sem.at[c, part, h],
            )
            for h in range(halves)
            for part in range(2)
        ]
        for c in range(chunks)
    ]
    for group in loads:
        for copy in group:
            copy.start()

    barrier = pltpu.get_barrier_semaphore()
    for d in range(1, groups):
        pl.semaphore_signal(
            barrier, inc=1, device_id={"freq": freq_peer(d)}, device_id_type=MESH
        )
    for d in range(1, senses):
        pl.semaphore_signal(
            barrier, inc=1, device_id={"sens": sens_peer(d)}, device_id_type=MESH
        )
    has_left = k > 0
    has_right = k < params - 1

    @pl.when(has_left)
    def _():
        for d in range(groups):
            pl.semaphore_signal(
                barrier,
                inc=1,
                device_id={"freq": freq_peer(d), "param": k - 1},
                device_id_type=MESH,
            )

    @pl.when(has_right)
    def _():
        for d in range(groups):
            pl.semaphore_signal(
                barrier,
                inc=1,
                device_id={"freq": freq_peer(d), "param": k + 1},
                device_id_type=MESH,
            )

    small[0].wait()
    peers = groups + senses - 2
    beside = jnp.where(has_left, groups, 0) + jnp.where(has_right, groups, 0)
    pl.semaphore_wait(barrier, peers + beside)

    def series_copy(slot, target):
        return pltpu.make_async_remote_copy(
            src_ref=gathered.at[f],
            dst_ref=gathered.at[slot],
            send_sem=g_send.at[target],
            recv_sem=g_recv.at[slot],
            device_id={"freq": target},
            device_id_type=MESH,
        )

    for d in range(1, groups):
        series_copy(f, freq_peer(d)).start()
    for copy in small[1:]:
        copy.wait()
    probe_row = wide.shape[2]
    row = lax.broadcasted_iota(jnp.int32, (probe_row, wide.shape[3]), 0)
    lane = lax.broadcasted_iota(jnp.int32, (probe_row, wide.shape[3]), 1)
    probe = (row // (16 * keep)) % senses * keep + row % keep
    same = lane % probes == probe
    for v in range(2):
        for i in range(2):
            full = jnp.dot(pick[v], spec_tab[i], preferred_element_type=F32)
            wide[v, i] = jnp.where(same, full, 0.0).astype(BF16)
    row = lax.broadcasted_iota(jnp.int32, spread.shape, 0)
    lane = lax.broadcasted_iota(jnp.int32, spread.shape, 1)
    spread[...] = jnp.where(lane // 8 == row, 1.0, 0.0).astype(BF16)
    norm = 1.0 / math.sqrt(bins_dev * groups)
    row = lax.broadcasted_iota(jnp.int32, weight.shape[1:], 0)
    for h in range(halves):
        value = jnp.zeros(weight.shape[1:], F32)
        for b in range(8):
            value = jnp.where(row // (2 * keep) == b, prior[h * 8 + b] * norm, value)
        weight[h] = value

    for d in range(1, groups):
        series_copy(freq_peer(d), freq_peer(d)).wait_recv()
    rows = jnp.concatenate([gathered[g] for g in range(groups)], axis=0)
    row = lax.broadcasted_iota(jnp.int32, (block, spread.shape[1]), 0)
    lane = lax.broadcasted_iota(jnp.int32, (block, spread.shape[1]), 1)
    same = lane % 8 == row // (2 * keep) % 8
    for h in range(halves):
        for v in range(2):
            spec = jnp.dot(
                wide[v, 0, h * block : (h + 1) * block], rows, preferred_element_type=F32
            ) + jnp.dot(
                wide[v, 1, h * block : (h + 1) * block], rows, preferred_element_type=F32
            )
            full = jnp.dot(spec.astype(BF16), spread[...], preferred_element_type=F32)
            left_mat[v, h] = jnp.where(same, full, 0.0).astype(BF16)


    def z_copy(target, slot, c):
        return pltpu.make_async_remote_copy(
            src_ref=sbuf.at[target, c],
            dst_ref=rbuf.at[slot, c],
            send_sem=z_send.at[target, c],
            recv_sem=z_recv.at[slot, c],
            device_id={"sens": target},
            device_id_type=MESH,
        )

    paired = senses == 4
    if paired:
        pair = s + 1 - 2 * lax.rem(s, 2)
        across = senses - 1 - s
        other = senses - 1 - pair
        outer = jnp.logical_or(s == 0, s == senses - 1)
        inner = jnp.logical_not(outer)

        @pl.when(inner)
        def _():
            rbuf[other] = jnp.zeros(rbuf.shape[1:], BF16)

    def relay_copy(c):
        return pltpu.make_async_remote_copy(
            src_ref=sbuf.at[other, c],
            dst_ref=relay.at[c],
            send_sem=relay_send.at[c],
            recv_sem=relay_recv.at[c],
            device_id={"sens": pair},
            device_id_type=MESH,
        )

    def joined_copy(c):
        return pltpu.make_async_remote_copy(
            src_ref=joined.at[c],
            dst_ref=rbuf.at[s, c],
            send_sem=z_send.at[across, c],
            recv_sem=z_recv.at[s, c],
            device_id={"sens": across},
            device_id_type=MESH,
        )

    def send_sums(c):
        if not paired:
            for d in range(1, senses):
                z_copy(sens_peer(d), s, c).start()
            return

        @pl.when(outer)
        def _():
            relay_copy(c).start()
            z_copy(across, s, c).start()
            z_copy(pair, s, c).start()

        @pl.when(inner)
        def _():
            z_copy(other, s, c).start()
            z_copy(pair, s, c).start()

    def pass_on(c):
        if not paired or c >= chunks:
            return

        @pl.when(inner)
        def _():
            relay_copy(c).wait_recv()
            both = sbuf[across, c].astype(F32) + relay[c].astype(F32)
            joined[c] = both.astype(BF16)
            joined_copy(c).start()

    def collect(c):
        total = sbuf[s, c].astype(F32)
        if not paired:
            for d in range(1, senses):
                z_copy(sens_peer(d), sens_peer(d), c).wait_recv()
                total = total + rbuf[sens_peer(d), c].astype(F32)
            return total
        z_copy(pair, pair, c).wait_recv()

        @pl.when(outer)
        def _():
            z_copy(other, other, c).wait_recv()

        z_copy(across, across, c).wait_recv()
        for slot in (pair, other, across):
            total = total + rbuf[slot, c].astype(F32)
        return total

    def drain(c):
        if not paired:
            for d in range(1, senses):
                z_copy(sens_peer(d), s, c).wait_send()
            return

        @pl.when(outer)
        def _():
            relay_copy(c).wait_send()
            z_copy(across, s, c).wait_send()
            z_copy(pair, s, c).wait_send()

        @pl.when(inner)
        def _():
            z_copy(other, s, c).wait_send()
            z_copy(pair, s, c).wait_send()
            joined_copy(c).wait_send()

    for c in range(chunks):
        for h in range(halves):
            total = jnp.zeros((block, width), F32)
            for part in range(2):
                loads[c][h * 2 + part].wait()
                right_mat = kbuf.at[c, part, h].reshape(sens_dev * 8, width)[...]
                total = total + jnp.dot(
                    left_mat[part, h], right_mat, preferred_element_type=F32
                )
            each = block // senses
            for j in range(senses):
                piece = total[j * each : (j + 1) * each] * weight[h]
                sbuf[j, c, h * each : (h + 1) * each, :] = piece.astype(BF16)
        send_sums(c)

    def x_copy(target, slot, c):
        return pltpu.make_async_remote_copy(
            src_ref=xsend.at[target, c],
            dst_ref=xrecv.at[slot, c],
            send_sem=x_send.at[target, c],
            recv_sem=x_recv.at[slot, c],
            device_id={"freq": target},
            device_id_type=MESH,
        )

    def to_left(target, slot):
        return pltpu.make_async_remote_copy(
            src_ref=xsend.at[target, 0, :, pl.ds(0, edge)],
            dst_ref=halo_right.at[slot],
            send_sem=hl_send.at[target],
            recv_sem=hr_recv.at[slot],
            device_id={"freq": target, "param": jnp.maximum(k - 1, 0)},
            device_id_type=MESH,
        )

    def to_right(target, slot):
        return pltpu.make_async_remote_copy(
            src_ref=xsend.at[target, chunks - 1, :, pl.ds(width - edge, edge)],
            dst_ref=halo_left.at[slot],
            send_sem=hr_send.at[target],
            recv_sem=hl_recv.at[slot],
            device_id={"freq": target, "param": jnp.minimum(k + 1, params - 1)},
            device_id_type=MESH,
        )

    pass_on(0)
    for c in range(chunks):
        pass_on(c + 1)
        total = collect(c)
        high = total.astype(BF16)
        low = (total - high.astype(F32)).astype(BF16)
        stacked = jnp.concatenate([high, high, low], axis=0)
        lanes = scale[:, c * width : (c + 1) * width]
        for d in list(range(1, groups)) + [0]:
            g = freq_peer(d)
            image = jnp.dot(img_tab[g], stacked, preferred_element_type=F32) * lanes
            if d == 0:
                own[c] = image
                if c == 0 or c == chunks - 1:
                    xsend[g, c] = image.astype(BF16)
            else:
                xsend[g, c] = image.astype(BF16)
                x_copy(g, f, c).start()
        if c == 0:

            @pl.when(has_left)
            def _():
                for d in range(groups):
                    to_left(freq_peer(d), f).start()

        if c == chunks - 1:

            @pl.when(has_right)
            def _():
                for d in range(groups):
                    to_right(freq_peer(d), f).start()

    for c in range(chunks):
        image = own[c]
        for d in range(1, groups):
            g = freq_peer(d)
            x_copy(g, g, c).wait_recv()
            image = image + xrecv[g, c].astype(F32)
        own[c] = image


    @pl.when(has_left)
    def _():
        for d in range(groups):
            to_right(freq_peer(d), freq_peer(d)).wait_recv()

    @pl.when(jnp.logical_not(has_left))
    def _():
        halo_left[...] = jnp.zeros_like(halo_left)

    @pl.when(has_right)
    def _():
        for d in range(groups):
            to_left(freq_peer(d), freq_peer(d)).wait_recv()

    @pl.when(jnp.logical_not(has_right))
    def _():
        halo_right[...] = jnp.zeros_like(halo_right)

    left = halo_left[0].astype(F32)
    right = halo_right[0].astype(F32)
    for g in range(1, groups):
        left = left + halo_left[g].astype(F32)
        right = right + halo_right[g].astype(F32)
    for c in range(chunks):
        mid = own[c]
        before = own[c - 1][:, width - 1 :] if c > 0 else left[:, edge - 1 :]
        after = own[c + 1][:, :1] if c < chunks - 1 else right[:, :1]
        lower = jnp.concatenate([before, mid[:, :-1]], axis=1)
        upper = jnp.concatenate([mid[:, 1:], after], axis=1)
        lanes = scale[:, c * width : (c + 1) * width]
        out_ref[:, c * width : (c + 1) * width] = lanes * (0.5 * mid + 0.25 * (lower + upper))

    for d in range(1, groups):
        series_copy(f, freq_peer(d)).wait_send()
        for c in range(chunks):
            x_copy(freq_peer(d), f, c).wait_send()
    for c in range(chunks):
        drain(c)

    @pl.when(has_left)
    def _():
        for d in range(groups):
            to_left(freq_peer(d), f).wait_send()

    @pl.when(has_right)
    def _():
        for d in range(groups):
            to_right(freq_peer(d), f).wait_send()


def local(mesh_shape, series, kernel, prior_spectrum, prior_scale):
    groups, params, senses = (mesh_shape[n] for n in ("freq", "param", "sens"))
    probes, sens_dev, time_dev = series.shape
    _, bins_dev, _, cols = kernel.shape
    keep = probes // senses
    chunks = 4
    width = cols // chunks
    edge = min(128, width)
    rows = time_dev * keep
    depth = bins_dev * 2 * keep
    halves = bins_dev // 8
    block = 16 * probes
    spec_tab = spectrum_tables(groups, bins_dev, time_dev, probes)
    pick_tab = pick_tables(bins_dev, senses, keep)
    img_tab = image_tables(groups, bins_dev, time_dev, keep)
    dma = pltpu.SemaphoreType.DMA
    out = pl.pallas_call(
        functools.partial(body, (groups, params, senses, chunks)),
        out_shape=jax.ShapeDtypeStruct((rows, cols), F32),
        in_specs=[pl.BlockSpec(memory_space=pltpu.HBM)] * 7,
        out_specs=pl.BlockSpec(memory_space=pltpu.VMEM),
        scratch_shapes=[
            pltpu.VMEM((chunks, 2, halves, sens_dev, 8, width), BF16),
            pltpu.SMEM((bins_dev,), F32),
            pltpu.VMEM((1, cols), F32),
            pltpu.VMEM(spec_tab.shape[1:], BF16),
            pltpu.VMEM(img_tab.shape[1:], BF16),
            pltpu.VMEM(pick_tab.shape, BF16),
            pltpu.VMEM((groups, time_dev * probes, sens_dev), BF16),
            pltpu.VMEM((2, 2, halves * block, groups * time_dev * probes), BF16),
            pltpu.VMEM((sens_dev, sens_dev * 8), BF16),
            pltpu.VMEM((2, halves, block, sens_dev * 8), BF16),
            pltpu.VMEM((halves, block // senses, width), F32),
            pltpu.VMEM((senses, chunks, depth, width), BF16),
            pltpu.VMEM((senses, chunks, depth, width), BF16),
            pltpu.VMEM((chunks, depth, width), BF16),
            pltpu.VMEM((chunks, depth, width), BF16),
            pltpu.VMEM((chunks, rows, width), F32),
            pltpu.VMEM((groups, chunks, rows, width), BF16),
            pltpu.VMEM((groups, chunks, rows, width), BF16),
            pltpu.VMEM((groups, rows, edge), BF16),
            pltpu.VMEM((groups, rows, edge), BF16),
            dma((6,)),
            dma((chunks, 2, halves)),
            dma((groups,)),
            dma((groups,)),
            dma((senses, chunks)),
            dma((senses, chunks)),
            dma((chunks,)),
            dma((chunks,)),
            dma((groups, chunks)),
            dma((groups, chunks)),
            dma((groups,)),
            dma((groups,)),
            dma((groups,)),
            dma((groups,)),
        ],
        compiler_params=pltpu.CompilerParams(
            collective_id=0, has_side_effects=True, vmem_limit_bytes=60 * 1024 * 1024
        ),
    )(
        series.transpose(2, 0, 1).reshape(time_dev * probes, sens_dev),
        kernel.transpose(0, 2, 1, 3),
        prior_spectrum,
        prior_scale.reshape(1, cols),
        jnp.asarray(spec_tab),
        jnp.asarray(img_tab),
        jnp.asarray(pick_tab),
    )
    return out.reshape(time_dev, keep, cols)


def solution(mesh):
    placed = (P(None, "sens", "freq"), P(None, "freq", "sens", "param"), P("freq"), P("param"))
    return jax.shard_map(
        functools.partial(local, dict(mesh.shape)),
        mesh=mesh,
        in_specs=placed,
        out_specs=P("freq", "sens", "param"),
        check_vma=False,
    )
```
